32 devices in a mesh: seq: 8 (over z, y), dp: 4 (over x, core).
Axes of the slice: x: 2, y: 2, z: 4, core: 2. Of those that a mesh axis runs over, the one named last changes fastest.
Arguments:
- hidden: bfloat16 [4, 2048, 4608], P('dp', 'seq'), may hold values from -6 to 6
- queries: bfloat16 [4, 2048, 2048], P('dp', 'seq'), may hold values from -64 to 64
- down_weight: bfloat16 [4608, 1024], P('dp'), may hold values from -0.09375 to 0.09375
- up_weight: bfloat16 [2, 512, 1024], P(None, 'dp'), may hold values from -0.25 to 0.25
- lengths: int32 [4], P('dp'), may hold values from 512 to 2048
Outputs:
- latent_cache: bfloat16 [4, 2048, 1024], P('dp', 'seq')
- attended: bfloat16 [4, 2048, 2048], P('dp', 'seq')
The draws below stay inside these ranges and needn't reach their ends.
All inputs are finite; a program needn't handle non-finite values.
Results may differ from the reference program's by a relative error of at most 0.012.
The reference program's roundings to bfloat16 on the way count: a program that leaves them out, or rounds other values in their place, can miss the bound.
Values may be sent and summed in bfloat16 or wider, within the bound.
A program may use at most 128 MiB of HBM per device.

```python
import math
import jax
import jax.numpy as jnp
from jax import lax

D = 4608
HEAD = 128
Q_HEADS = 16
KV_HEADS = 8
RANK = 1024
WINDOW = 4096
SEQ = 2048
BATCH = 4


def draw_queries(key, part):
    base_key = jax.random.fold_in(key, 11)
    entry_key, scale_key = jax.random.split(base_key)
    entries = jnp.clip(jax.random.normal(entry_key, (BATCH, SEQ, Q_HEADS, HEAD), jnp.float32), -4.0, 4.0)
    lowest, highest = (0.5, 16.0)
    log_scales = jax.random.uniform(scale_key, (BATCH, SEQ, Q_HEADS, 1), jnp.float32, math.log(lowest), math.log(highest))
    scaled = entries * jnp.exp(log_scales)
    return scaled.reshape(BATCH, SEQ, Q_HEADS * HEAD).astype(jnp.bfloat16)


def plant(drawn, stream_key, low, largest):
    extent = drawn.shape
    place = [jax.random.randint(jax.random.fold_in(stream_key, axis), (), 0, extent[axis]) for axis in range(len(extent))]
    drawn = drawn.at[tuple(place)].set(low)
    longest = extent.index(max(extent))
    place[longest] = (place[longest] + 1) % extent[longest]
    return drawn.at[tuple(place)].set(largest)


def block_levels(stream_key, extent, pieces, least, high):
    gain, own = 1.0, jax.random.fold_in(stream_key, 6)
    for dim, parts in pieces:
        steps = jnp.exp(jax.random.uniform(jax.random.fold_in(own, dim), (parts,), jnp.float32, least / len(pieces), high / len(pieces)))
        gain = gain * jnp.repeat(steps, extent[dim] // parts).reshape([-1 if axis == dim else 1 for axis in range(len(extent))])
    return gain


def bell_draw(rng, shape, scale, bound, pieces=(), kind=jnp.bfloat16):
    values = jax.random.normal(rng, shape, jnp.float32) * scale
    if len(pieces) > 0:
        values = block_levels(rng, shape, pieces, -0.22, 0.18) * values
    return jnp.clip(values, min=-bound, max=bound).astype(kind)


def setup_inputs(seed: int = 0) -> dict:
    arg_keys = jax.random.split(jax.random.key(seed), 6)
    return {
        "hidden": bell_draw(arg_keys[0], (BATCH, SEQ, D), 1.0, 6.0, ((0, 4), (1, 8))),
        "queries": draw_queries(jax.random.fold_in(arg_keys[5], 71), 0),
        "down_weight": bell_draw(arg_keys[2], (D, RANK), D ** -0.5, 0.09375, ((0, 4),)),
        "up_weight": bell_draw(arg_keys[3], (2, RANK // 2, KV_HEADS * HEAD), (RANK // 2) ** -0.5, 0.25, ((1, 4),)),
        "lengths": plant(jax.random.randint(arg_keys[4], (BATCH,), SEQ // 4, SEQ + 1), jax.random.fold_in(arg_keys[4], 1), SEQ // 4, SEQ).astype(jnp.int32),
    }


query_scale = 144.0 ** -0.5
soft_cap = 50.0


def rotate(values_in, start_pos):
    batches, count, width = values_in.shape
    half_head = HEAD // 2
    places = (start_pos + jnp.arange(count, dtype=jnp.int32)).astype(jnp.float32)
    freqs = 10000.0 ** (-2.0 * jnp.arange(half_head, dtype=jnp.float32) / HEAD)
    angles = places[:, None] * freqs[None, :]
    cosine = jnp.cos(angles)[None, :, None, :]
    sine_val = jnp.sin(angles)[None, :, None, :]
    split_heads = values_in.reshape(batches, count, width // HEAD, 2, half_head)
    lower = split_heads[:, :, :, 0, :]
    upper = split_heads[:, :, :, 1, :]
    turned = jnp.stack([lower * cosine - upper * sine_val, upper * cosine + lower * sine_val], axis=3)
    return turned.reshape(batches, count, width)


def reference(hidden, queries, down_weight, up_weight, lengths):
    flat_hidden = hidden.reshape(BATCH * SEQ, D)
    latent = jnp.dot(flat_hidden, down_weight, preferred_element_type=jnp.float32).astype(jnp.bfloat16)
    latent = latent.reshape(BATCH, SEQ, RANK)
    positions = jnp.arange(SEQ, dtype=jnp.int32)
    is_live = positions[None, :] < lengths[:, None]
    latent = jnp.where(is_live[:, :, None], latent, jnp.zeros((), jnp.bfloat16))
    key_rank = RANK // 2
    kv_width = KV_HEADS * HEAD
    keys_raw = jnp.dot(latent[:, :, :key_rank].reshape(-1, key_rank), up_weight[0], preferred_element_type=jnp.float32)
    keys_all = rotate(keys_raw.reshape(BATCH, SEQ, kv_width), 0).astype(jnp.bfloat16)
    values_all = jnp.dot(latent[:, :, key_rank:].reshape(-1, key_rank), up_weight[1], preferred_element_type=jnp.float32)
    values_all = values_all.astype(jnp.bfloat16).reshape(BATCH, SEQ, kv_width)
    block_rows = math.gcd(512, SEQ)
    blocks = SEQ // block_rows
    padding = jnp.zeros((BATCH, WINDOW, kv_width), jnp.bfloat16)
    keys_pad = jnp.concatenate([padding, keys_all], axis=1)
    values_pad = jnp.concatenate([padding, values_all], axis=1)
    query_width = Q_HEADS * HEAD
    ratio = Q_HEADS // KV_HEADS

    def one_block(flat_index):
        batch_index = (flat_index // blocks).astype(jnp.int32)
        row_start = ((flat_index % blocks) * block_rows).astype(jnp.int32)
        zero_idx = jnp.zeros((), jnp.int32)
        keys_win = lax.dynamic_slice(keys_pad, (batch_index, row_start, zero_idx), (1, WINDOW + block_rows, kv_width))[0]
        values_win = lax.dynamic_slice(values_pad, (batch_index, row_start, zero_idx), (1, WINDOW + block_rows, kv_width))[0]
        query_blk = lax.dynamic_slice(queries, (batch_index, row_start, zero_idx), (1, block_rows, query_width))[0]
        q_split = query_blk.astype(jnp.float32).reshape(block_rows, KV_HEADS, ratio, HEAD)
        keys_grp = keys_win.astype(jnp.float32).reshape(-1, KV_HEADS, HEAD)
        values_grp = values_win.astype(jnp.float32).reshape(-1, KV_HEADS, HEAD)
        raw = jnp.einsum("lgrd,ngd->grln", q_split, keys_grp, precision=lax.Precision.HIGHEST)
        capped = soft_cap * jnp.tanh(raw * (query_scale / soft_cap))
        q_pos = row_start + jnp.arange(block_rows, dtype=jnp.int32)
        key_pos = row_start - WINDOW + jnp.arange(WINDOW + block_rows, dtype=jnp.int32)
        allowed = (key_pos[None, :] <= q_pos[:, None]) & (key_pos[None, :] > q_pos[:, None] - WINDOW) & (key_pos[None, :] >= 0)
        expo = jnp.where(allowed, jnp.exp(capped), 0.0)
        denom = jnp.sum(expo, axis=-1)
        probs = expo.astype(jnp.bfloat16).astype(jnp.float32)
        numer = jnp.einsum("grln,ngd->lgrd", probs, values_grp, precision=lax.Precision.HIGHEST)
        result = numer / jnp.transpose(denom, (2, 0, 1))[..., None]
        result = result.reshape(block_rows, query_width)
        live_rows = q_pos < lengths[batch_index]
        return jnp.where(live_rows[:, None], result, 0.0).astype(jnp.bfloat16)

    outputs = lax.map(one_block, jnp.arange(BATCH * blocks, dtype=jnp.int32))
    attended = outputs.reshape(BATCH, SEQ, query_width)
    return latent, attended
```

```python
import functools
import math

import jax
import jax.numpy as jnp
import numpy as np
from jax import lax
from jax.experimental import pallas as pl
from jax.experimental.pallas import tpu as pltpu
from jax.sharding import PartitionSpec as P

HEAD = 128
WINDOW = 4096
MESH = pl.DeviceIdType.MESH

query_scale = 144.0 ** (-0.5)
soft_cap = 50.0
EXP_SCALE = soft_cap * math.log2(math.e)


def angle_tables(rows, blocks):
    half = HEAD // 2
    freqs = 10000.0 ** (-2.0 * np.arange(half, dtype=np.float64) / HEAD)
    freqs = np.concatenate([freqs, freqs])[None, :]
    sign = np.concatenate([-np.ones(half), np.ones(half)])[None, :]
    near = np.arange(rows, dtype=np.float64)[:, None] * freqs
    far = (rows * np.arange(blocks, dtype=np.float64))[:, None] * freqs
    near = np.stack([np.cos(near), sign * np.sin(near)]).astype(np.float32)
    far = np.stack([np.cos(far), sign * np.sin(far)]).astype(np.float32)
    return near, far

UP_PIECES = 2
PARTS = 8
LATE = 5


def kernel(
    ring, lengths_ref, hidden_ref, q_ref, down_ref, up_ref, near_ref, far_ref,
    latent_out, attended_out,
    hid, far_hid, q_raw, qs, wf, up, part_out, part_in, lat, acc, keys, values, numer, denom, out_buf,
    local_sem, own_send, own_recv, h_send, h_recv, p_send, p_recv,
    x_send, x_recv, y_send, y_recv, z_send, z_recv, c_send, c_recv, um_send, um_recv,
    chain_send, pair_send, lat_recv, out_sem,
):
    seq = lax.axis_index("seq")
    dp = lax.axis_index("dp")
    rows = lat.shape[1]
    shard = down_ref.shape[0]
    chip_k = 2 * shard
    part_rows = rows // PARTS
    up_rows = up_ref.shape[1]
    up_half = up_rows // 2
    up_piece = up_half // UP_PIECES
    groups = qs.shape[0]
    ratio = qs.shape[1] // rows
    key_rank = lat.shape[2] // 2
    total = ring * rows

    side = lax.rem(seq, 2)
    pair = seq + 1 - 2 * side
    level = lax.rem(seq // 2, 2)
    fellow = seq + 2 - 4 * level
    core = lax.rem(dp, 2)
    mate = dp + 1 - 2 * core
    across = lax.rem(dp + 2, 4)
    has_next = seq + 2 < ring

    def local(src, dst, sem):
        return pltpu.make_async_copy(src, dst, sem)

    def k_range(owner):
        return pl.ds(pl.multiple_of(owner // 2 * chip_k, 128), chip_k)

    own_weight = pl.ds(pl.multiple_of(core * shard, 128), shard)

    def up_view(owner, kv, half, index):
        start = owner * up_rows + half * up_half + index * up_piece
        return up.at[kv, pl.ds(pl.multiple_of(start, up_piece), up_piece)]

    def up_shard(owner):
        return up.at[:, pl.ds(pl.multiple_of(owner * up_rows, up_rows), up_rows), :]

    loads = [
        local(down_ref, wf.at[own_weight], local_sem.at[0]),
        local(hidden_ref.at[0, :, k_range(dp)], hid, local_sem.at[1]),
        local(up_ref, up_shard(dp), local_sem.at[2]),
        local(q_ref.at[0], q_raw, local_sem.at[3]),
    ]
    for load in loads:
        load.start()

    barrier = pltpu.get_barrier_semaphore()

    def greet(device):
        pl.semaphore_signal(barrier, inc=1, device_id=device, device_id_type=MESH)

    greet({"seq": seq, "dp": mate})
    greet({"seq": seq, "dp": across})
    greet({"seq": pair, "dp": dp})

    neighbours = 3
    for step in (2, 4, -2, -4):
        exists = (seq + step >= 0) & (seq + step < ring)
        neighbours = neighbours + exists.astype(jnp.int32)

        @pl.when(exists)
        def _(step=step):
            greet({"seq": seq + step, "dp": dp})

    pl.semaphore_wait(barrier, neighbours)

    def remote(src, dst, send, recv, device):
        return pltpu.make_async_remote_copy(
            src_ref=src, dst_ref=dst, send_sem=send, recv_sem=recv, device_id=device, device_id_type=MESH
        )

    to_mate = {"seq": seq, "dp": mate}
    to_across = {"seq": seq, "dp": across}
    to_pair = {"seq": pair, "dp": dp}
    to_fellow = {"seq": fellow, "dp": dp}

    def part_span(p):
        return pl.ds(pl.multiple_of(p * part_rows, part_rows), part_rows)

    def hidden_copy(p):
        return remote(
            hidden_ref.at[0, part_span(p), k_range(across)], far_hid.at[part_span(p)],
            h_send.at[p], h_recv.at[p], to_across,
        )

    def partial_copy(p):
        span = part_span(p)
        return remote(part_out.at[span], part_in.at[span], p_send.at[p], p_recv.at[p], to_across)

    hidden_copy(0).start()
    own_copy = remote(down_ref, wf.at[own_weight], own_send, own_recv, to_mate)
    own_copy.start()

    quarters = ((side, level), (1 - side, level), (side, 1 - level), (1 - side, 1 - level))

    def x_copy(i):
        kv, half = quarters[0]
        start = half * up_half + i * up_piece
        src = up_ref.at[kv, pl.ds(pl.multiple_of(start, up_piece), up_piece)]
        return remote(src, up_view(dp, kv, half, i), x_send.at[i], x_recv.at[i], to_across)

    def y_copy(which, slot):
        view = up_view(across, *quarters[which], slot % UP_PIECES)
        return remote(view, view, y_send.at[slot], y_recv.at[slot], to_pair)

    def z_copy(which, slot):
        view = up_view(across, *quarters[which], slot % UP_PIECES)
        return remote(view, view, z_send.at[slot], z_recv.at[slot], to_fellow)

    def c_copy(which, i):
        view = up_view(across, *quarters[which], i)
        return remote(view, view, c_send.at[which, i], c_recv.at[which, i], to_mate)

    x_copies = [x_copy(i) for i in range(UP_PIECES)]
    for copy in x_copies:
        copy.start()
    hidden_copy(1).start()
    up_mate = remote(up_ref, up_shard(dp), um_send, um_recv, to_mate)
    up_mate.start()
    y_copies = [y_copy(0, i) for i in range(UP_PIECES)]
    z_copies = [z_copy(0, i) for i in range(UP_PIECES)]
    relays = [y_copy(2, UP_PIECES), z_copy(1, UP_PIECES + 1)]
    mate_copies = [[c_copy(which, i) for i in range(UP_PIECES)] for which in range(4)]

    loads[3].wait()
    for g in range(groups):
        for r in range(ratio):
            column = (g * ratio + r) * HEAD
            qs[g, r * rows : (r + 1) * rows, :] = q_raw[:, column : column + HEAD]
    numer[...] = jnp.zeros_like(numer)
    denom[...] = jnp.zeros_like(denom)

    live_count = lengths_ref[0] - seq * rows

    def return_partial(p):
        hidden_copy(p).wait_recv()
        product = jnp.dot(far_hid[part_span(p)], wf[...], preferred_element_type=jnp.float32)
        part_out[part_span(p)] = product.astype(jnp.bfloat16)
        partial_copy(p).start()

    def chain(block, p, step):
        view = lat.at[block, part_span(p)]
        target = {"seq": lax.rem(seq + step, ring), "dp": dp}
        return remote(view, view, chain_send.at[step // 2 - 1, block, p], lat_recv.at[block, p], target)

    def swap(block, p):
        view = lat.at[block, part_span(p)]
        return remote(view, view, pair_send.at[block, p], lat_recv.at[block, p], to_pair)

    def climb(block, p, distance, act):
        for step in (2, 4):

            @pl.when((lax.rem(distance, 4) == 0) & (seq + step < ring))
            def _():
                act(chain(block, p, step))

    def cross(block, p, act):
        @pl.when((block == seq) & (side == 0) | (block < seq) & ((p < LATE) | (block > 0)))
        def _():
            act(swap(block, p))

    def start(copy):
        copy.start()

    def wait_send(copy):
        copy.wait_send()

    def finish_part(p):
        partial_copy(p).wait_recv()
        span = part_span(p)
        summed = acc[span] + part_in[span].astype(jnp.float32)
        position = lax.broadcasted_iota(jnp.int32, summed.shape, 0) + p * part_rows
        lat[seq, span] = jnp.where(position < live_count, summed, 0.0).astype(jnp.bfloat16)
        climb(seq, p, 0, start)
        cross(seq, p, start)

    def receive_same(block, p):
        swap(block, p).wait_recv()
        climb(block, p, seq - block, start)
        cross(block, p, start)

    def receive_other(block, p):
        swap(block, p).wait_recv()

        @pl.when((block == 0) & (side == 1) & (p >= LATE))
        def _():
            climb(block, p, seq - 1, start)

    def attend(pieces, size, mode):
        latents, cosines, sines = [], [], []
        for block, start in pieces:
            span = pl.ds(pl.multiple_of(start, size), size)
            latents.append(lat[block, span, :])
            near_cos, near_sin = near_ref[0, span, :], near_ref[1, span, :]
            far_cos = far_ref[0, pl.ds(block, 1), :]
            far_sin = far_ref[1, pl.ds(block, 1), :]
            cosines.append(near_cos * far_cos - near_sin * far_sin)
            sines.append(near_sin * far_cos + near_cos * far_sin)
        latent = jnp.concatenate(latents, axis=0)
        cosine = jnp.concatenate(cosines, axis=0)
        sine = jnp.concatenate(sines, axis=0)
        keys_raw = jnp.dot(latent[:, :key_rank], up[0], preferred_element_type=jnp.float32)
        for g in range(groups):
            head = keys_raw[:, g * HEAD : (g + 1) * HEAD]
            turned = head * cosine + pltpu.roll(head, HEAD // 2, 1) * sine
            keys[g] = turned.astype(jnp.bfloat16)
        values_raw = jnp.dot(latent[:, key_rank:], up[1], preferred_element_type=jnp.float32)
        for g in range(groups):
            values[g] = values_raw[:, g * HEAD : (g + 1) * HEAD].astype(jnp.bfloat16)
        if mode:
            shape = (rows, rows)
            column = lax.broadcasted_iota(jnp.int32, shape, 1)
            offset = jnp.zeros(shape, jnp.int32)
            for n, (block, start) in enumerate(pieces):
                base = (seq - block) * rows - start + n * size
                offset = jnp.where(column >= n * size, base, offset)
            gap = lax.broadcasted_iota(jnp.int32, shape, 0) - column + offset
            allowed = (gap >= 0) & (gap < WINDOW)
            allowed = jnp.concatenate([allowed.astype(jnp.float32)] * ratio, axis=0)
        for g in range(groups):
            raw = lax.dot_general(
                qs[g], keys[g], (((1,), (1,)), ((), ())), preferred_element_type=jnp.float32
            )
            expo = jnp.exp2(EXP_SCALE * jnp.tanh(raw * (query_scale / soft_cap)))
            if mode:
                expo = expo * allowed
            partial = expo[:, :HEAD]
            for column in range(HEAD, rows, HEAD):
                partial = partial + expo[:, column : column + HEAD]
            denom[g] += partial
            numer[g] += jnp.dot(expo.astype(jnp.bfloat16), values[g], preferred_element_type=jnp.float32)

    def attend_unit(u, carry):
        pieces = []
        for n in range(PARTS):
            index = u * PARTS + n
            p = sum((index >= m * seq).astype(jnp.int32) for m in range(1, PARTS))
            pieces.append((seq - 1 - (index - p * seq), p * part_rows))
        attend(pieces, part_rows, total > WINDOW)
        return carry

    loads[0].wait()
    own_copy.wait_recv()
    return_partial(0)
    hidden_copy(2).start()
    loads[1].wait()
    acc[...] = jnp.dot(hid[...], wf[...], preferred_element_type=jnp.float32)
    for i in range(UP_PIECES):
        x_copies[i].wait_recv()
        y_copies[i].start()
        z_copies[i].start()
        mate_copies[0][i].start()

    def spread_up():
        y_copies[0].wait_recv()
        mate_copies[1][0].start()
        z_copies[0].wait_recv()
        relays[0].start()
        mate_copies[2][0].start()
        y_copies[1].wait_recv()
        relays[1].start()
        mate_copies[1][1].start()
        z_copies[1].wait_recv()
        mate_copies[2][1].start()

    def collect_up():
        for i in range(UP_PIECES):
            relays[i].wait_recv()
            mate_copies[3][i].start()
        up_mate.wait_recv()
        loads[2].wait()
        for copies in mate_copies:
            for copy in copies:
                copy.wait_recv()

    latent_copy = local(lat.at[seq], latent_out.at[0], out_sem.at[groups])
    depth = (seq + 1) // 2
    last_slot = PARTS + depth // 2

    def slot(t, done):
        @pl.when(t < PARTS)
        def _():
            finish_part(t)

        @pl.when(t + 1 < PARTS)
        def _():
            return_partial(t + 1)

        @pl.when(t + 3 < PARTS)
        def _():
            hidden_copy(t + 3).start()

        @pl.when(t == 0)
        def _():
            spread_up()

        def visit(j, carry):
            same, other = seq - 2 * j - 2, seq - 2 * j - 1
            p_same, p_other = t - 1 - j // 2, t - 1 - (j + 1) // 2

            @pl.when((same >= 0) & (p_same >= 0) & (p_same < PARTS))
            def _():
                receive_same(same, p_same)

            @pl.when((p_other >= 0) & (p_other < PARTS))
            def _():
                receive_other(other, p_other)

            return carry

        lax.fori_loop(0, depth, visit, 0)

        @pl.when(t == 2)
        def _():
            collect_up()

        @pl.when(t == PARTS)
        def _():
            latent_copy.start()

        @pl.when(t == jnp.where(has_next, last_slot, PARTS))
        def _():
            attend([(seq, 0)], rows, True)

        complete = jnp.clip(t - depth // 2, 0, PARTS) * seq // PARTS
        upto = jnp.where(has_next, 0, jnp.minimum(complete, done + 1))
        upto = jnp.where(t == last_slot, seq, upto)
        lax.fori_loop(done, upto, attend_unit, 0)
        return upto

    lax.fori_loop(0, last_slot + 1, slot, 0)

    live_rows = lax.broadcasted_iota(jnp.int32, (rows, HEAD), 0) < live_count
    width = ratio * HEAD
    for g in range(groups):
        result = numer[g] / jnp.sum(denom[g], axis=1, keepdims=True)
        for r in range(ratio):
            column = g * width + r * HEAD
            piece_out = jnp.where(live_rows, result[r * rows : (r + 1) * rows], 0.0)
            out_buf[:, column : column + HEAD] = piece_out.astype(jnp.bfloat16)
        columns = pl.ds(g * width, width)
        local(out_buf.at[:, columns], attended_out.at[0, :, columns], out_sem.at[g]).start()

    def drain(k, carry):
        block = seq - 2 * k

        def drain_part(p, inner):
            climb(block, p, 2 * k, wait_send)
            cross(block, p, wait_send)
            return inner

        return lax.fori_loop(0, PARTS, drain_part, carry)

    lax.fori_loop(0, seq // 2 + 1, drain, 0)

    def drain_late(p, carry):
        @pl.when(side == 1)
        def _():
            climb(0, p, seq - 1, wait_send)

        return carry

    lax.fori_loop(LATE, PARTS, drain_late, 0)

    for p in range(PARTS):
        hidden_copy(p).wait_send()
        partial_copy(p).wait_send()
    sent = x_copies + y_copies + z_copies + relays + sum(mate_copies, [])
    for copy in sent + [own_copy, up_mate]:
        copy.wait_send()
    latent_copy.wait()
    for g in range(groups):
        columns = pl.ds(g * width, width)
        local(out_buf.at[:, columns], attended_out.at[0, :, columns], out_sem.at[g]).wait()


def body(ring, dp_size, hidden, queries, down_weight, up_weight, lengths):
    _, rows, model_dim = hidden.shape
    shard, rank = down_weight.shape
    kv_width = up_weight.shape[2]
    groups = kv_width // HEAD
    q_width = queries.shape[2]
    ratio = q_width // kv_width
    near, far = angle_tables(rows, ring)
    any_spec = pl.BlockSpec(memory_space=pl.ANY)
    vmem_spec = pl.BlockSpec(memory_space=pltpu.VMEM)
    f32, bf16, dma = jnp.float32, jnp.bfloat16, pltpu.SemaphoreType.DMA
    return pl.pallas_call(
        functools.partial(kernel, ring),
        out_shape=(
            jax.ShapeDtypeStruct((1, rows, rank), bf16),
            jax.ShapeDtypeStruct((1, rows, q_width), bf16),
        ),
        in_specs=[pl.BlockSpec(memory_space=pltpu.SMEM)] + [any_spec] * 4 + [vmem_spec] * 2,
        out_specs=(any_spec, any_spec),
        scratch_shapes=[
            pltpu.VMEM((rows, 2 * shard), bf16),
            pltpu.VMEM((rows, 2 * shard), bf16),
            pltpu.VMEM((rows, q_width), bf16),
            pltpu.VMEM((groups, ratio * rows, HEAD), bf16),
            pltpu.VMEM((2 * shard, rank), bf16),
            pltpu.VMEM((2, dp_size * up_weight.shape[1], kv_width), bf16),
            pltpu.VMEM((rows, rank), bf16),
            pltpu.VMEM((rows, rank), bf16),
            pltpu.VMEM((ring, rows, rank), bf16),
            pltpu.VMEM((rows, rank), f32),
            pltpu.VMEM((groups, rows, HEAD), bf16),
            pltpu.VMEM((groups, rows, HEAD), bf16),
            pltpu.VMEM((groups, ratio * rows, HEAD), f32),
            pltpu.VMEM((groups, ratio * rows, HEAD), f32),
            pltpu.VMEM((rows, q_width), bf16),
            dma((4,)),
            dma, dma,
            dma((PARTS,)), dma((PARTS,)),
            dma((PARTS,)), dma((PARTS,)),
            dma((UP_PIECES,)), dma((UP_PIECES,)),
            dma((2 * UP_PIECES,)), dma((2 * UP_PIECES,)),
            dma((2 * UP_PIECES,)), dma((2 * UP_PIECES,)),
            dma((4, UP_PIECES)), dma((4, UP_PIECES)),
            dma, dma,
            dma((2, ring, PARTS)), dma((ring, PARTS)), dma((ring, PARTS)),
            dma((groups + 1,)),
        ],
        compiler_params=pltpu.CompilerParams(
            collective_id=0, has_side_effects=True, vmem_limit_bytes=60 * 1024 * 1024
        ),
    )(lengths, hidden, queries, down_weight, up_weight, jnp.asarray(near), jnp.asarray(far))


def solution(mesh):
    in_specs = (
        P("dp", "seq", None),
        P("dp", "seq", None),
        P("dp", None),
        P(None, "dp", None),
        P("dp"),
    )
    out_specs = (P("dp", "seq", None), P("dp", "seq", None))
    step = functools.partial(body, mesh.shape["seq"], mesh.shape["dp"])
    return jax.shard_map(step, mesh=mesh, in_specs=in_specs, out_specs=out_specs, check_vma=False)
```

```python
import functools
import math

import jax
import jax.numpy as jnp
import numpy as np
from jax import lax
from jax.experimental import pallas as pl
from jax.experimental.pallas import tpu as pltpu
from jax.sharding import PartitionSpec as P

HEAD = 128
WINDOW = 4096
MESH = pl.DeviceIdType.MESH

query_scale = 144.0 ** (-0.5)
soft_cap = 50.0
EXP_SCALE = soft_cap * math.log2(math.e)


def angle_tables(rows, blocks):
    half = HEAD // 2
    freqs = 10000.0 ** (-2.0 * np.arange(half, dtype=np.float64) / HEAD)
    freqs = np.concatenate([freqs, freqs])[None, :]
    sign = np.concatenate([-np.ones(half), np.ones(half)])[None, :]
    near = np.arange(rows, dtype=np.float64)[:, None] * freqs
    far = (rows * np.arange(blocks, dtype=np.float64))[:, None] * freqs
    near = np.stack([np.cos(near), sign * np.sin(near)]).astype(np.float32)
    far = np.stack([np.cos(far), sign * np.sin(far)]).astype(np.float32)
    return near, far

UP_PIECES = 2
VMEM_BYTES = 67043328
SPARE_BYTES = 32768
PARTS = 8
LATE = 4
EAGER = 7


def kernel(
    ring, lengths_hbm, hidden_ref, q_ref, down_ref, up_ref, near_hbm, far_hbm,
    latent_out, attended_out,
    lengths_ref, near_ref, far_ref, hid, far_hid, q_raw, qs, wf, up, part_out, part_in, lat, acc, keys, values, numer, denom,
    local_sem, own_send, own_recv, h_send, h_recv, p_send, p_recv,
    x_send, x_recv, y_send, y_recv, z_send, z_recv, c_send, c_recv, um_send, um_recv,
    chain_send, pair_send, lat_recv,
):
    seq = lax.axis_index("seq")
    dp = lax.axis_index("dp")
    rows = lat.shape[1]
    shard = down_ref.shape[0]
    chip_k = 2 * shard
    part_rows = rows // PARTS
    up_rows = up_ref.shape[1]
    up_half = up_rows // 2
    up_piece = up_half // UP_PIECES
    groups = qs.shape[0]
    ratio = qs.shape[1] // rows
    key_rank = lat.shape[2] // 2
    total = ring * rows

    side = lax.rem(seq, 2)
    pair = seq + 1 - 2 * side
    level = lax.rem(seq // 2, 2)
    fellow = seq + 2 - 4 * level
    core = lax.rem(dp, 2)
    mate = dp + 1 - 2 * core
    across = lax.rem(dp + 2, 4)
    has_next = seq + 2 < ring

    def local(src, dst, sem):
        return pltpu.make_async_copy(src, dst, sem)

    def k_range(owner):
        return pl.ds(pl.multiple_of(owner // 2 * chip_k, 128), chip_k)

    own_weight = pl.ds(pl.multiple_of(core * shard, 128), shard)

    def up_view(owner, kv, half, index):
        start = owner * up_rows + half * up_half + index * up_piece
        return up.at[kv, pl.ds(pl.multiple_of(start, up_piece), up_piece)]

    def up_shard(owner):
        return up.at[:, pl.ds(pl.multiple_of(owner * up_rows, up_rows), up_rows), :]

    loads = [
        local(down_ref, wf.at[own_weight], local_sem.at[0]),
        local(hidden_ref.at[0, :, k_range(dp)], hid, local_sem.at[1]),
        local(up_ref, up_shard(dp), local_sem.at[2]),
        local(q_ref.at[0], q_raw, local_sem.at[3]),
        local(near_hbm, near_ref, local_sem.at[4]),
        local(far_hbm, far_ref, local_sem.at[5]),
        local(lengths_hbm, lengths_ref, local_sem.at[6]),
    ]
    for load in loads:
        load.start()

    barrier = pltpu.get_barrier_semaphore()

    def greet(device):
        pl.semaphore_signal(barrier, inc=1, device_id=device, device_id_type=MESH)

    greet({"seq": seq, "dp": mate})
    greet({"seq": seq, "dp": across})
    greet({"seq": pair, "dp": dp})

    neighbours = 3
    for step in (2, 4, -2, -4):
        exists = (seq + step >= 0) & (seq + step < ring)
        neighbours = neighbours + exists.astype(jnp.int32)

        @pl.when(exists)
        def _(step=step):
            greet({"seq": seq + step, "dp": dp})

    pl.semaphore_wait(barrier, neighbours)

    def remote(src, dst, send, recv, device):
        return pltpu.make_async_remote_copy(
            src_ref=src, dst_ref=dst, send_sem=send, recv_sem=recv, device_id=device, device_id_type=MESH
        )

    to_mate = {"seq": seq, "dp": mate}
    to_across = {"seq": seq, "dp": across}
    to_pair = {"seq": pair, "dp": dp}
    to_fellow = {"seq": fellow, "dp": dp}

    def part_span(p):
        return pl.ds(pl.multiple_of(p * part_rows, part_rows), part_rows)

    def hidden_copy(p):
        return remote(
            hidden_ref.at[0, part_span(p), k_range(across)], far_hid.at[part_span(p)],
            h_send.at[p], h_recv.at[p], to_across,
        )

    def partial_copy(p):
        span = part_span(p)
        return remote(part_out.at[span], part_in.at[span], p_send.at[p], p_recv.at[p], to_across)

    hidden_copy(0).start()
    own_copy = remote(down_ref, wf.at[own_weight], own_send, own_recv, to_mate)
    own_copy.start()

    quarters = ((side, level), (1 - side, level), (side, 1 - level), (1 - side, 1 - level))

    def x_copy(i):
        kv, half = quarters[0]
        start = half * up_half + i * up_piece
        src = up_ref.at[kv, pl.ds(pl.multiple_of(start, up_piece), up_piece)]
        return remote(src, up_view(dp, kv, half, i), x_send.at[i], x_recv.at[i], to_across)

    def y_copy(which, slot):
        view = up_view(across, *quarters[which], slot % UP_PIECES)
        return remote(view, view, y_send.at[slot], y_recv.at[slot], to_pair)

    def z_copy(which, slot):
        view = up_view(across, *quarters[which], slot % UP_PIECES)
        return remote(view, view, z_send.at[slot], z_recv.at[slot], to_fellow)

    def c_copy(which, i):
        view = up_view(across, *quarters[which], i)
        return remote(view, view, c_send.at[which, i], c_recv.at[which, i], to_mate)

    x_copies = [x_copy(i) for i in range(UP_PIECES)]
    for copy in x_copies:
        copy.start()
    hidden_copy(1).start()
    up_mate = remote(up_ref, up_shard(dp), um_send, um_recv, to_mate)
    up_mate.start()
    y_copies = [y_copy(0, i) for i in range(UP_PIECES)]
    z_copies = [z_copy(0, i) for i in range(UP_PIECES)]
    relays = [y_copy(2, UP_PIECES), z_copy(1, UP_PIECES + 1)]
    mate_copies = [[c_copy(which, i) for i in range(UP_PIECES)] for which in range(4)]

    for load in loads[3:]:
        load.wait()
    for g in range(groups):
        for r in range(ratio):
            column = (g * ratio + r) * HEAD
            qs[g, r * rows : (r + 1) * rows, :] = q_raw[:, column : column + HEAD]
    numer[...] = jnp.zeros_like(numer)
    denom[...] = jnp.zeros_like(denom)

    live_count = lengths_ref[0] - seq * rows

    def return_partial(p):
        hidden_copy(p).wait_recv()
        product = jnp.dot(far_hid[part_span(p)], wf[...], preferred_element_type=jnp.float32)
        part_out[part_span(p)] = product.astype(jnp.bfloat16)
        partial_copy(p).start()

    def chain(block, p, step):
        view = lat.at[block, part_span(p)]
        target = {"seq": lax.rem(seq + step, ring), "dp": dp}
        return remote(view, view, chain_send.at[step // 2 - 1, block, p], lat_recv.at[block, p], target)

    def swap(block, p):
        view = lat.at[block, part_span(p)]
        return remote(view, view, pair_send.at[block, p], lat_recv.at[block, p], to_pair)

    def climb(block, p, distance, act):
        for step in (2, 4):

            @pl.when((lax.rem(distance, 4) == 0) & (seq + step < ring))
            def _():
                act(chain(block, p, step))

    def cross(block, p, act):
        @pl.when((block == seq) & (side == 0) | (block < seq) & ((p < LATE) | (block > 0)))
        def _():
            act(swap(block, p))

    def start(copy):
        copy.start()

    def wait_send(copy):
        copy.wait_send()

    def finish_part(p):
        partial_copy(p).wait_recv()
        span = part_span(p)
        summed = acc[span] + part_in[span].astype(jnp.float32)
        position = lax.broadcasted_iota(jnp.int32, summed.shape, 0) + p * part_rows
        lat[seq, span] = jnp.where(position < live_count, summed, 0.0).astype(jnp.bfloat16)
        climb(seq, p, 0, start)
        cross(seq, p, start)

    def receive_same(block, p):
        swap(block, p).wait_recv()
        climb(block, p, seq - block, start)
        cross(block, p, start)

    def receive_other(block, p):
        swap(block, p).wait_recv()

        @pl.when((block == 0) & (side == 1) & (p >= LATE))
        def _():
            climb(block, p, seq - 1, start)

    def attend(pieces, size, mode):
        latents, cosines, sines = [], [], []
        for block, start in pieces:
            span = pl.ds(pl.multiple_of(start, size), size)
            latents.append(lat[block, span, :])
            near_cos, near_sin = near_ref[0, span, :], near_ref[1, span, :]
            far_cos = far_ref[0, pl.ds(block, 1), :]
            far_sin = far_ref[1, pl.ds(block, 1), :]
            cosines.append(near_cos * far_cos - near_sin * far_sin)
            sines.append(near_sin * far_cos + near_cos * far_sin)
        latent = jnp.concatenate(latents, axis=0)
        cosine = jnp.concatenate(cosines, axis=0)
        sine = jnp.concatenate(sines, axis=0)
        keys_raw = jnp.dot(latent[:, :key_rank], up[0], preferred_element_type=jnp.float32)
        for g in range(groups):
            head = keys_raw[:, g * HEAD : (g + 1) * HEAD]
            turned = head * cosine + pltpu.roll(head, HEAD // 2, 1) * sine
            keys[g] = turned.astype(jnp.bfloat16)
        values_raw = jnp.dot(latent[:, key_rank:], up[1], preferred_element_type=jnp.float32)
        for g in range(groups):
            values[g] = values_raw[:, g * HEAD : (g + 1) * HEAD].astype(jnp.bfloat16)
        if mode:
            shape = (rows, rows)
            column = lax.broadcasted_iota(jnp.int32, shape, 1)
            offset = jnp.zeros(shape, jnp.int32)
            for n, (block, start) in enumerate(pieces):
                base = (seq - block) * rows - start + n * size
                offset = jnp.where(column >= n * size, base, offset)
            gap = lax.broadcasted_iota(jnp.int32, shape, 0) - column + offset
            allowed = (gap >= 0) & (gap < WINDOW)
            allowed = jnp.concatenate([allowed.astype(jnp.float32)] * ratio, axis=0)
        for g in range(groups):
            raw = lax.dot_general(
                qs[g], keys[g], (((1,), (1,)), ((), ())), preferred_element_type=jnp.float32
            )
            expo = jnp.exp2(EXP_SCALE * jnp.tanh(raw * (query_scale / soft_cap)))
            if mode:
                expo = expo * allowed
            partial = expo[:, :HEAD]
            for column in range(HEAD, rows, HEAD):
                partial = partial + expo[:, column : column + HEAD]
            denom[g] += partial
            numer[g] += jnp.dot(expo.astype(jnp.bfloat16), values[g], preferred_element_type=jnp.float32)

    def attend_unit(u, carry):
        pieces = []
        for n in range(PARTS):
            index = u * PARTS + n
            p = sum((index >= m * seq).astype(jnp.int32) for m in range(1, PARTS))
            pieces.append((seq - 1 - (index - p * seq), p * part_rows))
        attend(pieces, part_rows, total > WINDOW)
        return carry

    loads[0].wait()
    own_copy.wait_recv()
    return_partial(0)
    hidden_copy(2).start()
    loads[1].wait()
    acc[...] = jnp.dot(hid[...], wf[...], preferred_element_type=jnp.float32)
    for i in range(UP_PIECES):
        x_copies[i].wait_recv()
        y_copies[i].start()
        z_copies[i].start()
        mate_copies[0][i].start()

    def spread_up():
        y_copies[0].wait_recv()
        mate_copies[1][0].start()
        z_copies[0].wait_recv()
        relays[0].start()
        mate_copies[2][0].start()
        y_copies[1].wait_recv()
        relays[1].start()
        mate_copies[1][1].start()
        z_copies[1].wait_recv()
        mate_copies[2][1].start()

    def collect_up():
        for i in range(UP_PIECES):
            relays[i].wait_recv()
            mate_copies[3][i].start()
        up_mate.wait_recv()
        loads[2].wait()
        for copies in mate_copies:
            for copy in copies:
                copy.wait_recv()

    depth = (seq + 1) // 2
    last_slot = PARTS + depth // 2

    def slot(t, done):
        @pl.when(t < PARTS)
        def _():
            finish_part(t)

        @pl.when(t + 1 < PARTS)
        def _():
            return_partial(t + 1)

        @pl.when(t + 3 < PARTS)
        def _():
            hidden_copy(t + 3).start()

        @pl.when(t == 0)
        def _():
            spread_up()

        def visit(j, carry):
            same, other = seq - 2 * j - 2, seq - 2 * j - 1
            p_same, p_other = t - 1 - j // 2, t - 1 - (j + 1) // 2

            @pl.when((same >= 0) & (p_same >= 0) & (p_same < PARTS))
            def _():
                receive_same(same, p_same)

            @pl.when((p_other >= 0) & (p_other < PARTS))
            def _():
                receive_other(other, p_other)

            return carry

        near_visits = jnp.minimum(depth, 1)
        lax.fori_loop(0, near_visits, visit, 0)
        complete = jnp.clip(t - 1 - depth // 2, 0, PARTS) * seq // PARTS
        upto = jnp.where(has_next & (t < EAGER), 0, jnp.minimum(complete, done + 1))
        lax.fori_loop(done, upto, attend_unit, 0)
        lax.fori_loop(near_visits, depth, visit, 0)

        @pl.when(t == 2)
        def _():
            collect_up()

        @pl.when(t == PARTS)
        def _():
            attend([(seq, 0)], rows, True)

        return upto

    attended_units = lax.fori_loop(0, last_slot + 1, slot, 0)
    lax.fori_loop(attended_units, seq, attend_unit, 0)

    live_rows = lax.broadcasted_iota(jnp.int32, (rows, HEAD), 0) < live_count
    width = ratio * HEAD
    for g in range(groups):
        result = numer[g] / jnp.sum(denom[g], axis=1, keepdims=True)
        for r in range(ratio):
            column = g * width + r * HEAD
            piece_out = jnp.where(live_rows, result[r * rows : (r + 1) * rows], 0.0)
            attended_out[0, :, column : column + HEAD] = piece_out.astype(jnp.bfloat16)
    latent_out[0] = lat[seq]

    def drain(k, carry):
        block = seq - 2 * k

        def drain_part(p, inner):
            climb(block, p, 2 * k, wait_send)
            cross(block, p, wait_send)
            return inner

        return lax.fori_loop(0, PARTS, drain_part, carry)

    lax.fori_loop(0, seq // 2 + 1, drain, 0)

    def drain_late(p, carry):
        @pl.when(side == 1)
        def _():
            climb(0, p, seq - 1, wait_send)

        return carry

    lax.fori_loop(LATE, PARTS, drain_late, 0)

    for p in range(PARTS):
        hidden_copy(p).wait_send()
        partial_copy(p).wait_send()
    sent = x_copies + y_copies + z_copies + relays + sum(mate_copies, [])
    for copy in sent + [own_copy, up_mate]:
        copy.wait_send()


def deliver(latent_ref, attended_ref, latent_out, attended_out, sem):
    copies = [
        pltpu.make_async_copy(attended_ref, attended_out, sem.at[0]),
        pltpu.make_async_copy(latent_ref, latent_out, sem.at[1]),
    ]
    for copy in copies:
        copy.start()
    for copy in copies:
        copy.wait()


def body(ring, dp_size, hidden, queries, down_weight, up_weight, lengths):
    _, rows, model_dim = hidden.shape
    shard, rank = down_weight.shape
    kv_width = up_weight.shape[2]
    groups = kv_width // HEAD
    q_width = queries.shape[2]
    ratio = q_width // kv_width
    near, far = angle_tables(rows, ring)
    any_spec = pl.BlockSpec(memory_space=pl.ANY)
    vmem_spec = pl.BlockSpec(memory_space=pltpu.VMEM)
    f32, bf16, dma = jnp.float32, jnp.bfloat16, pltpu.SemaphoreType.DMA
    latent, attended = pl.pallas_call(
        functools.partial(kernel, ring),
        out_shape=(
            pltpu.VMEM((1, rows, rank), bf16),
            pltpu.VMEM((1, rows, q_width), bf16),
        ),
        in_specs=[pl.BlockSpec(memory_space=pltpu.HBM)] * 7,
        out_specs=(vmem_spec, vmem_spec),
        scratch_shapes=[
            pltpu.SMEM(lengths.shape, jnp.int32),
            pltpu.VMEM(near.shape, f32),
            pltpu.VMEM(far.shape, f32),
            pltpu.VMEM((rows, 2 * shard), bf16),
            pltpu.VMEM((rows, 2 * shard), bf16),
            pltpu.VMEM((rows, q_width), bf16),
            pltpu.VMEM((groups, ratio * rows, HEAD), bf16),
            pltpu.VMEM((2 * shard, rank), bf16),
            pltpu.VMEM((2, dp_size * up_weight.shape[1], kv_width), bf16),
            pltpu.VMEM((rows, rank), bf16),
            pltpu.VMEM((rows, rank), bf16),
            pltpu.VMEM((ring, rows, rank), bf16),
            pltpu.VMEM((rows, rank), f32),
            pltpu.VMEM((groups, rows, HEAD), bf16),
            pltpu.VMEM((groups, rows, HEAD), bf16),
            pltpu.VMEM((groups, ratio * rows, HEAD), f32),
            pltpu.VMEM((groups, ratio * rows, HEAD), f32),
            dma((7,)),
            dma, dma,
            dma((PARTS,)), dma((PARTS,)),
            dma((PARTS,)), dma((PARTS,)),
            dma((UP_PIECES,)), dma((UP_PIECES,)),
            dma((2 * UP_PIECES,)), dma((2 * UP_PIECES,)),
            dma((2 * UP_PIECES,)), dma((2 * UP_PIECES,)),
            dma((4, UP_PIECES)), dma((4, UP_PIECES)),
            dma, dma,
            dma((2, ring, PARTS)), dma((ring, PARTS)), dma((ring, PARTS)),
        ],
        compiler_params=pltpu.CompilerParams(
            collective_id=0, has_side_effects=True, vmem_limit_bytes=VMEM_BYTES - 2 * rows * (rank + q_width) - SPARE_BYTES
        ),
    )(lengths, hidden, queries, down_weight, up_weight, jnp.asarray(near), jnp.asarray(far))
    return pl.pallas_call(
        deliver,
        out_shape=(
            jax.ShapeDtypeStruct((1, rows, rank), bf16),
            jax.ShapeDtypeStruct((1, rows, q_width), bf16),
        ),
        in_specs=[vmem_spec, vmem_spec],
        out_specs=(any_spec, any_spec),
        scratch_shapes=[dma((2,))],
        compiler_params=pltpu.CompilerParams(vmem_limit_bytes=8 * 1024 * 1024),
    )(latent, attended)


def solution(mesh):
    in_specs = (
        P("dp", "seq", None),
        P("dp", "seq", None),
        P("dp", None),
        P(None, "dp", None),
        P("dp"),
    )
    out_specs = (P("dp", "seq", None), P("dp", "seq", None))
    step = functools.partial(body, mesh.shape["seq"], mesh.shape["dp"])
    return jax.shard_map(step, mesh=mesh, in_specs=in_specs, out_specs=out_specs, check_vma=False)
```

```python
import functools
import math

import jax
import jax.numpy as jnp
import numpy as np
from jax import lax
from jax.experimental import pallas as pl
from jax.experimental.pallas import tpu as pltpu
from jax.sharding import PartitionSpec as P

HEAD = 128
WINDOW = 4096
MESH = pl.DeviceIdType.MESH

query_scale = 144.0 ** (-0.5)
soft_cap = 50.0
EXP_SCALE = soft_cap * math.log2(math.e)


def angle_tables(rows, blocks):
    half = HEAD // 2
    freqs = 10000.0 ** (-2.0 * np.arange(half, dtype=np.float64) / HEAD)
    freqs = np.concatenate([freqs, freqs])[None, :]
    sign = np.concatenate([-np.ones(half), np.ones(half)])[None, :]
    near = np.arange(rows, dtype=np.float64)[:, None] * freqs
    far = (rows * np.arange(blocks, dtype=np.float64))[:, None] * freqs
    near = np.stack([np.cos(near), sign * np.sin(near)]).astype(np.float32)
    far = np.stack([np.cos(far), sign * np.sin(far)]).astype(np.float32)
    return near, far

UP_PIECES = 2
VMEM_BYTES = 67043328
SPARE_BYTES = 32768
PARTS = 8
LATE = 5
EAGER = 6


def kernel(
    ring, lengths_hbm, hidden_ref, q_ref, down_ref, up_ref, near_hbm, far_hbm,
    latent_out, attended_out,
    lengths_ref, near_ref, far_ref, hid, far_hid, q_raw, qs, wf, up, part_out, part_in, lat, acc, keys, values, numer, denom,
    local_sem, own_send, own_recv, h_send, h_recv, p_send, p_recv,
    x_send, x_recv, y_send, y_recv, z_send, z_recv, c_send, c_recv, um_send, um_recv,
    chain_send, pair_send, lat_recv,
):
    seq = lax.axis_index("seq")
    dp = lax.axis_index("dp")
    rows = lat.shape[1]
    shard = down_ref.shape[0]
    chip_k = 2 * shard
    part_rows = rows // PARTS
    up_rows = up_ref.shape[1]
    up_half = up_rows // 2
    up_piece = up_half // UP_PIECES
    groups = qs.shape[0]
    ratio = qs.shape[1] // rows
    key_rank = lat.shape[2] // 2
    total = ring * rows

    side = lax.rem(seq, 2)
    pair = seq + 1 - 2 * side
    level = lax.rem(seq // 2, 2)
    fellow = seq + 2 - 4 * level
    core = lax.rem(dp, 2)
    mate = dp + 1 - 2 * core
    across = lax.rem(dp + 2, 4)
    has_next = seq + 2 < ring

    def local(src, dst, sem):
        return pltpu.make_async_copy(src, dst, sem)

    def k_range(owner):
        return pl.ds(pl.multiple_of(owner // 2 * chip_k, 128), chip_k)

    own_weight = pl.ds(pl.multiple_of(core * shard, 128), shard)

    def up_view(owner, kv, half, index):
        start = owner * up_rows + half * up_half + index * up_piece
        return up.at[kv, pl.ds(pl.multiple_of(start, up_piece), up_piece)]

    def up_shard(owner):
        return up.at[:, pl.ds(pl.multiple_of(owner * up_rows, up_rows), up_rows), :]

    loads = [
        local(down_ref, wf.at[own_weight], local_sem.at[0]),
        local(hidden_ref.at[0, :, k_range(dp)], hid, local_sem.at[1]),
        local(up_ref, up_shard(dp), local_sem.at[2]),
        local(q_ref.at[0], q_raw, local_sem.at[3]),
        local(near_hbm, near_ref, local_sem.at[4]),
        local(far_hbm, far_ref, local_sem.at[5]),
        local(lengths_hbm, lengths_ref, local_sem.at[6]),
    ]
    for load in loads:
        load.start()

    barrier = pltpu.get_barrier_semaphore()

    def greet(device):
        pl.semaphore_signal(barrier, inc=1, device_id=device, device_id_type=MESH)

    greet({"seq": seq, "dp": mate})
    greet({"seq": seq, "dp": across})
    greet({"seq": pair, "dp": dp})

    neighbours = 3
    for step in (2, 4, -2, -4):
        exists = (seq + step >= 0) & (seq + step < ring)
        neighbours = neighbours + exists.astype(jnp.int32)

        @pl.when(exists)
        def _(step=step):
            greet({"seq": seq + step, "dp": dp})

    pl.semaphore_wait(barrier, neighbours)

    def remote(src, dst, send, recv, device):
        return pltpu.make_async_remote_copy(
            src_ref=src, dst_ref=dst, send_sem=send, recv_sem=recv, device_id=device, device_id_type=MESH
        )

    to_mate = {"seq": seq, "dp": mate}
    to_across = {"seq": seq, "dp": across}
    to_pair = {"seq": pair, "dp": dp}
    to_fellow = {"seq": fellow, "dp": dp}

    def part_span(p):
        return pl.ds(pl.multiple_of(p * part_rows, part_rows), part_rows)

    def hidden_copy(p):
        return remote(
            hidden_ref.at[0, part_span(p), k_range(across)], far_hid.at[part_span(p)],
            h_send.at[p], h_recv.at[p], to_across,
        )

    def partial_copy(p):
        span = part_span(p)
        return remote(part_out.at[span], part_in.at[span], p_send.at[p], p_recv.at[p], to_across)

    hidden_copy(0).start()
    own_copy = remote(down_ref, wf.at[own_weight], own_send, own_recv, to_mate)
    own_copy.start()

    quarters = ((side, level), (1 - side, level), (side, 1 - level), (1 - side, 1 - level))

    def x_copy(i):
        kv, half = quarters[0]
        start = half * up_half + i * up_piece
        src = up_ref.at[kv, pl.ds(pl.multiple_of(start, up_piece), up_piece)]
        return remote(src, up_view(dp, kv, half, i), x_send.at[i], x_recv.at[i], to_across)

    def y_copy(which, slot):
        view = up_view(across, *quarters[which], slot % UP_PIECES)
        return remote(view, view, y_send.at[slot], y_recv.at[slot], to_pair)

    def z_copy(which, slot):
        view = up_view(across, *quarters[which], slot % UP_PIECES)
        return remote(view, view, z_send.at[slot], z_recv.at[slot], to_fellow)

    def c_copy(which, i):
        view = up_view(across, *quarters[which], i)
        return remote(view, view, c_send.at[which, i], c_recv.at[which, i], to_mate)

    x_copies = [x_copy(i) for i in range(UP_PIECES)]
    for copy in x_copies:
        copy.start()
    hidden_copy(1).start()
    up_mate = remote(up_ref, up_shard(dp), um_send, um_recv, to_mate)
    up_mate.start()
    y_copies = [y_copy(0, i) for i in range(UP_PIECES)]
    z_copies = [z_copy(0, i) for i in range(UP_PIECES)]
    relays = [y_copy(2, UP_PIECES), z_copy(1, UP_PIECES + 1)]
    mate_copies = [[c_copy(which, i) for i in range(UP_PIECES)] for which in range(4)]

    for load in loads[3:]:
        load.wait()
    for g in range(groups):
        for r in range(ratio):
            column = (g * ratio + r) * HEAD
            qs[g, r * rows : (r + 1) * rows, :] = q_raw[:, column : column + HEAD]
    numer[...] = jnp.zeros_like(numer)
    denom[...] = jnp.zeros_like(denom)

    live_count = lengths_ref[0] - seq * rows

    def return_partial(p):
        hidden_copy(p).wait_recv()
        product = jnp.dot(far_hid[part_span(p)], wf[...], preferred_element_type=jnp.float32)
        part_out[part_span(p)] = product.astype(jnp.bfloat16)
        partial_copy(p).start()

    def chain(block, p, step):
        view = lat.at[block, part_span(p)]
        target = {"seq": lax.rem(seq + step, ring), "dp": dp}
        return remote(view, view, chain_send.at[step // 2 - 1, block, p], lat_recv.at[block, p], target)

    def swap(block, p):
        view = lat.at[block, part_span(p)]
        return remote(view, view, pair_send.at[block, p], lat_recv.at[block, p], to_pair)

    def climb(block, p, distance, act):
        for step in (2, 4):

            @pl.when((lax.rem(distance, 4) == 0) & (seq + step < ring))
            def _():
                act(chain(block, p, step))

    def cross(block, p, act):
        @pl.when((block == seq) & (side == 0) | (block < seq) & ((p < LATE) | (block > 0)))
        def _():
            act(swap(block, p))

    def start(copy):
        copy.start()

    def wait_send(copy):
        copy.wait_send()

    def finish_part(p):
        partial_copy(p).wait_recv()
        span = part_span(p)
        summed = acc[span] + part_in[span].astype(jnp.float32)
        position = lax.broadcasted_iota(jnp.int32, summed.shape, 0) + p * part_rows
        lat[seq, span] = jnp.where(position < live_count, summed, 0.0).astype(jnp.bfloat16)
        climb(seq, p, 0, start)
        cross(seq, p, start)

    def receive_same(block, p):
        swap(block, p).wait_recv()
        climb(block, p, seq - block, start)
        cross(block, p, start)

    def receive_other(block, p):
        swap(block, p).wait_recv()

        @pl.when((block == 0) & (side == 1) & (p >= LATE))
        def _():
            climb(block, p, seq - 1, start)

    def attend(pieces, size, mode):
        latents, cosines, sines = [], [], []
        for block, start in pieces:
            span = pl.ds(pl.multiple_of(start, size), size)
            latents.append(lat[block, span, :])
            near_cos, near_sin = near_ref[0, span, :], near_ref[1, span, :]
            far_cos = far_ref[0, pl.ds(block, 1), :]
            far_sin = far_ref[1, pl.ds(block, 1), :]
            cosines.append(near_cos * far_cos - near_sin * far_sin)
            sines.append(near_sin * far_cos + near_cos * far_sin)
        latent = jnp.concatenate(latents, axis=0)
        cosine = jnp.concatenate(cosines, axis=0)
        sine = jnp.concatenate(sines, axis=0)
        keys_raw = jnp.dot(latent[:, :key_rank], up[0], preferred_element_type=jnp.float32)
        for g in range(groups):
            head = keys_raw[:, g * HEAD : (g + 1) * HEAD]
            turned = head * cosine + pltpu.roll(head, HEAD // 2, 1) * sine
            keys[g] = turned.astype(jnp.bfloat16)
        values_raw = jnp.dot(latent[:, key_rank:], up[1], preferred_element_type=jnp.float32)
        for g in range(groups):
            values[g] = values_raw[:, g * HEAD : (g + 1) * HEAD].astype(jnp.bfloat16)
        if mode:
            shape = (rows, rows)
            column = lax.broadcasted_iota(jnp.int32, shape, 1)
            offset = jnp.zeros(shape, jnp.int32)
            for n, (block, start) in enumerate(pieces):
                base = (seq - block) * rows - start + n * size
                offset = jnp.where(column >= n * size, base, offset)
            gap = lax.broadcasted_iota(jnp.int32, shape, 0) - column + offset
            allowed = (gap >= 0) & (gap < WINDOW)
            allowed = jnp.concatenate([allowed.astype(jnp.float32)] * ratio, axis=0)
        for g in range(groups):
            raw = lax.dot_general(
                qs[g], keys[g], (((1,), (1,)), ((), ())), preferred_element_type=jnp.float32
            )
            expo = jnp.exp2(EXP_SCALE * jnp.tanh(raw * (query_scale / soft_cap)))
            if mode:
                expo = expo * allowed
            partial = expo[:, :HEAD]
            for column in range(HEAD, rows, HEAD):
                partial = partial + expo[:, column : column + HEAD]
            denom[g] += partial
            numer[g] += jnp.dot(expo.astype(jnp.bfloat16), values[g], preferred_element_type=jnp.float32)

    def attend_unit(u, carry):
        pieces = []
        for n in range(PARTS):
            index = u * PARTS + n
            p = sum((index >= m * seq).astype(jnp.int32) for m in range(1, PARTS))
            pieces.append((seq - 1 - (index - p * seq), p * part_rows))
        attend(pieces, part_rows, total > WINDOW)
        return carry

    loads[0].wait()
    own_copy.wait_recv()
    return_partial(0)
    hidden_copy(2).start()
    loads[1].wait()
    acc[...] = jnp.dot(hid[...], wf[...], preferred_element_type=jnp.float32)
    for i in range(UP_PIECES):
        x_copies[i].wait_recv()
        y_copies[i].start()
        z_copies[i].start()
        mate_copies[0][i].start()

    def spread_up():
        y_copies[0].wait_recv()
        mate_copies[1][0].start()
        z_copies[0].wait_recv()
        relays[0].start()
        mate_copies[2][0].start()
        y_copies[1].wait_recv()
        relays[1].start()
        mate_copies[1][1].start()
        z_copies[1].wait_recv()
        mate_copies[2][1].start()

    def collect_up():
        for i in range(UP_PIECES):
            relays[i].wait_recv()
            mate_copies[3][i].start()
        up_mate.wait_recv()
        loads[2].wait()
        for copies in mate_copies:
            for copy in copies:
                copy.wait_recv()

    depth = (seq + 1) // 2
    last_slot = PARTS + depth // 2 + 1

    def slot(t, done):
        @pl.when(t + 1 < PARTS)
        def _():
            return_partial(t + 1)

        @pl.when(t + 3 < PARTS)
        def _():
            hidden_copy(t + 3).start()

        @pl.when(t < PARTS)
        def _():
            finish_part(t)

        @pl.when(t == 0)
        def _():
            spread_up()

        def visit_same(j, carry):
            block, p = seq - 2 * j - 2, t - 1 - j // 2

            @pl.when((block >= 0) & (p >= 0) & (p < PARTS))
            def _():
                receive_same(block, p)

            return carry

        def visit_other(j, carry):
            p = t - 2 - (j + 1) // 2

            @pl.when((p >= 0) & (p < PARTS))
            def _():
                receive_other(seq - 2 * j - 1, p)

            return carry

        lax.fori_loop(0, depth, visit_same, 0)
        complete = jnp.clip(t - 2 - depth // 2, 0, PARTS) * seq // PARTS
        upto = jnp.where(has_next & (t < EAGER), 0, jnp.minimum(complete, done + 1))
        lax.fori_loop(done, upto, attend_unit, 0)
        lax.fori_loop(0, depth, visit_other, 0)

        @pl.when(t == 2)
        def _():
            collect_up()

        @pl.when(t == PARTS)
        def _():
            attend([(seq, 0)], rows, True)

        return upto

    attended_units = lax.fori_loop(0, last_slot + 1, slot, 0)
    lax.fori_loop(attended_units, seq, attend_unit, 0)

    live_rows = lax.broadcasted_iota(jnp.int32, (rows, HEAD), 0) < live_count
    width = ratio * HEAD
    for g in range(groups):
        result = numer[g] / jnp.sum(denom[g], axis=1, keepdims=True)
        for r in range(ratio):
            column = g * width + r * HEAD
            piece_out = jnp.where(live_rows, result[r * rows : (r + 1) * rows], 0.0)
            attended_out[0, :, column : column + HEAD] = piece_out.astype(jnp.bfloat16)
    latent_out[0] = lat[seq]

    def drain(k, carry):
        block = seq - 2 * k

        def drain_part(p, inner):
            climb(block, p, 2 * k, wait_send)
            cross(block, p, wait_send)
            return inner

        return lax.fori_loop(0, PARTS, drain_part, carry)

    lax.fori_loop(0, seq // 2 + 1, drain, 0)

    def drain_late(p, carry):
        @pl.when(side == 1)
        def _():
            climb(0, p, seq - 1, wait_send)

        return carry

    lax.fori_loop(LATE, PARTS, drain_late, 0)

    for p in range(PARTS):
        hidden_copy(p).wait_send()
        partial_copy(p).wait_send()
    sent = x_copies + y_copies + z_copies + relays + sum(mate_copies, [])
    for copy in sent + [own_copy, up_mate]:
        copy.wait_send()


def deliver(latent_ref, attended_ref, latent_out, attended_out, sem):
    copies = [
        pltpu.make_async_copy(attended_ref, attended_out, sem.at[0]),
        pltpu.make_async_copy(latent_ref, latent_out, sem.at[1]),
    ]
    for copy in copies:
        copy.start()
    for copy in copies:
        copy.wait()


def body(ring, dp_size, hidden, queries, down_weight, up_weight, lengths):
    _, rows, model_dim = hidden.shape
    shard, rank = down_weight.shape
    kv_width = up_weight.shape[2]
    groups = kv_width // HEAD
    q_width = queries.shape[2]
    ratio = q_width // kv_width
    near, far = angle_tables(rows, ring)
    any_spec = pl.BlockSpec(memory_space=pl.ANY)
    vmem_spec = pl.BlockSpec(memory_space=pltpu.VMEM)
    f32, bf16, dma = jnp.float32, jnp.bfloat16, pltpu.SemaphoreType.DMA
    latent, attended = pl.pallas_call(
        functools.partial(kernel, ring),
        out_shape=(
            pltpu.VMEM((1, rows, rank), bf16),
            pltpu.VMEM((1, rows, q_width), bf16),
        ),
        in_specs=[pl.BlockSpec(memory_space=pltpu.HBM)] * 7,
        out_specs=(vmem_spec, vmem_spec),
        scratch_shapes=[
            pltpu.SMEM(lengths.shape, jnp.int32),
            pltpu.VMEM(near.shape, f32),
            pltpu.VMEM(far.shape, f32),
            pltpu.VMEM((rows, 2 * shard), bf16),
            pltpu.VMEM((rows, 2 * shard), bf16),
            pltpu.VMEM((rows, q_width), bf16),
            pltpu.VMEM((groups, ratio * rows, HEAD), bf16),
            pltpu.VMEM((2 * shard, rank), bf16),
            pltpu.VMEM((2, dp_size * up_weight.shape[1], kv_width), bf16),
            pltpu.VMEM((rows, rank), bf16),
            pltpu.VMEM((rows, rank), bf16),
            pltpu.VMEM((ring, rows, rank), bf16),
            pltpu.VMEM((rows, rank), f32),
            pltpu.VMEM((groups, rows, HEAD), bf16),
            pltpu.VMEM((groups, rows, HEAD), bf16),
            pltpu.VMEM((groups, ratio * rows, HEAD), f32),
            pltpu.VMEM((groups, ratio * rows, HEAD), f32),
            dma((7,)),
            dma, dma,
            dma((PARTS,)), dma((PARTS,)),
            dma((PARTS,)), dma((PARTS,)),
            dma((UP_PIECES,)), dma((UP_PIECES,)),
            dma((2 * UP_PIECES,)), dma((2 * UP_PIECES,)),
            dma((2 * UP_PIECES,)), dma((2 * UP_PIECES,)),
            dma((4, UP_PIECES)), dma((4, UP_PIECES)),
            dma, dma,
            dma((2, ring, PARTS)), dma((ring, PARTS)), dma((ring, PARTS)),
        ],
        compiler_params=pltpu.CompilerParams(
            collective_id=0, has_side_effects=True, vmem_limit_bytes=VMEM_BYTES - 2 * rows * (rank + q_width) - SPARE_BYTES
        ),
    )(lengths, hidden, queries, down_weight, up_weight, jnp.asarray(near), jnp.asarray(far))
    return pl.pallas_call(
        deliver,
        out_shape=(
            jax.ShapeDtypeStruct((1, rows, rank), bf16),
            jax.ShapeDtypeStruct((1, rows, q_width), bf16),
        ),
        in_specs=[vmem_spec, vmem_spec],
        out_specs=(any_spec, any_spec),
        scratch_shapes=[dma((2,))],
        compiler_params=pltpu.CompilerParams(vmem_limit_bytes=8 * 1024 * 1024),
    )(latent, attended)


def solution(mesh):
    in_specs = (
        P("dp", "seq", None),
        P("dp", "seq", None),
        P("dp", None),
        P(None, "dp", None),
        P("dp"),
    )
    out_specs = (P("dp", "seq", None), P("dp", "seq", None))
    step = functools.partial(body, mesh.shape["seq"], mesh.shape["dp"])
    return jax.shard_map(step, mesh=mesh, in_specs=in_specs, out_specs=out_specs, check_vma=False)
```
